32 devices in a mesh: rep: 8 (over z, core), tp: 4 (over y, x).
Axes of the slice: x: 2, y: 2, z: 4, core: 2. Of those that a mesh axis runs over, the one named last changes fastest.
Arguments:
- hidden: bfloat16 [32, 4608], P('rep'), may hold values from -6 to 6
- positions: int32 [32], P('rep'), may hold values from 1 to 1023
- key_cache: bfloat16 [32, 16, 1024, 128], P('rep', 'tp'), may hold values from -6 to 6
- value_cache: bfloat16 [32, 16, 1024, 128], P('rep', 'tp'), may hold values from -6 to 6
- norm_gain: float32 [4608], replicated, may hold values from 0.1 to 1.9
- q_proj: bfloat16 [4096, 4608], P(('rep', 'tp')), may hold values from -0.09375 to 0.09375
- k_proj: bfloat16 [2048, 4608], P(('rep', 'tp')), may hold values from -0.09375 to 0.09375
- v_proj: bfloat16 [2048, 4608], P(('rep', 'tp')), may hold values from -0.09375 to 0.09375
- o_proj: bfloat16 [4608, 4096], P(('rep', 'tp')), may hold values from -0.09375 to 0.09375
- post_gain: float32 [4608], P('tp'), may hold values from 0.1 to 1.9
Outputs:
- joined_qkv: bfloat16 [4608, 8192], P(None, 'tp')
- wo_heads: bfloat16 [4096, 4608], P('tp')
- attn_out: bfloat16 [32, 4608], P('rep', 'tp')
The draws below stay inside these ranges and needn't reach their ends.
All inputs are finite; a program needn't handle non-finite values.
Results may differ from the reference program's by a relative error of at most 0.008.
Values may be sent and summed in bfloat16 or wider, within the bound.
A program may use at most 128 MiB of HBM per device.

```python
import jax
import jax.numpy as jnp
from jax import lax

D = 4608
HEADS = 32
KV_HEADS = 16
HEAD_DIM = 128
CTX = 1024
BATCH = 32
QKV_COLS = 8192
N_TP = 4


def touch_ends(entries, own_key, smallest, high):
    index_at = [jax.random.randint(jax.random.fold_in(own_key, axis), (), 0, length) for axis, length in enumerate(entries.shape)]
    main_axis = entries.shape.index(max(entries.shape))
    next_to = index_at[:main_axis] + [(index_at[main_axis] + 1) % entries.shape[main_axis]] + index_at[main_axis + 1:]
    return entries.at[tuple(index_at)].set(smallest).at[tuple(next_to)].set(high)


def block_scale(key, dims, pieces, low, high):
    def one(position, parts):
        draws = jax.random.uniform(jax.random.fold_in(jax.random.fold_in(key, 6), position), (parts,), jnp.float32, low / len(pieces), high / len(pieces))
        return jnp.repeat(jnp.exp(draws), dims[position] // parts).reshape((-1,) + (1,) * (len(dims) - position - 1))

    loudness = one(*pieces[0])
    for cut in pieces[1:]:
        loudness = loudness * one(*cut)
    return loudness


def normal_values(key, shape, deviation, limit, cuts=(), kind=jnp.bfloat16):
    entries = deviation * jax.random.normal(key, shape, jnp.float32)
    if cuts:
        entries = entries * block_scale(key, shape, cuts, -0.22, 0.18)
    return jnp.clip(entries, -limit, limit).astype(kind)


def setup_inputs(seed: int = 0) -> dict:
    arg_keys = jax.random.split(jax.random.key(seed), 11)
    return {
        "hidden": normal_values(arg_keys[0], (BATCH, D), 1.0, 6.0, ((0, 8),)),
        "positions": touch_ends(jax.random.randint(arg_keys[1], (BATCH,), 1, CTX), jax.random.fold_in(arg_keys[1], 1), 1, CTX - 1).astype(jnp.int32),
        "key_cache": normal_values(arg_keys[2], (BATCH, KV_HEADS, CTX, HEAD_DIM), 1.0, 6.0, ((0, 8), (1, 4))),
        "value_cache": normal_values(arg_keys[3], (BATCH, KV_HEADS, CTX, HEAD_DIM), 1.0, 6.0, ((0, 8), (1, 4))),
        "norm_gain": jnp.clip(1.0 + 0.18 * jax.random.normal(arg_keys[4], (D,), jnp.float32), 0.1, 1.9),
        "q_proj": normal_values(arg_keys[5], (HEADS * HEAD_DIM, D), D ** -0.5, 0.09375, ((0, 32),)),
        "k_proj": normal_values(arg_keys[6], (KV_HEADS * HEAD_DIM, D), D ** -0.5, 0.09375, ((0, 32),)),
        "v_proj": normal_values(arg_keys[7], (KV_HEADS * HEAD_DIM, D), D ** -0.5, 0.09375, ((0, 32),)),
        "o_proj": normal_values(arg_keys[8], (D, HEADS * HEAD_DIM), (HEADS * HEAD_DIM) ** -0.5, 0.09375, ((0, 32),)),
        "post_gain": jnp.clip(1.0 + 0.18 * jax.random.normal(arg_keys[9], (D,), jnp.float32), 0.1, 1.9),
    }


score_scale = 144.0 ** (-0.5)
soft_cap = 50.0

def rms_scale(values, gain):
    mean_square = lax.optimization_barrier(jnp.mean(values * values, axis=-1, keepdims=True))
    return values * lax.rsqrt(mean_square + 1e-06) * gain

def rotate(values, positions):
    half = values.shape[-1] // 2
    freq = 10000.0 ** (-2.0 * jnp.arange(half, dtype=jnp.float32) / values.shape[-1])
    angle = positions.astype(jnp.float32)[:, None] * freq[None, :]
    cosine = jnp.cos(angle)[:, None, :]
    sine = jnp.sin(angle)[:, None, :]
    first = values[..., :half]
    second = values[..., half:]
    return jnp.concatenate([first * cosine - second * sine, second * cosine + first * sine], axis=-1)

def reference(hidden, positions, key_cache, value_cache, norm_gain, q_proj, k_proj, v_proj, o_proj, post_gain):
    q_cols = jnp.transpose(q_proj).reshape(D, N_TP, -1)
    k_cols = jnp.transpose(k_proj).reshape(D, N_TP, -1)
    v_cols = jnp.transpose(v_proj).reshape(D, N_TP, -1)
    joined_qkv = jnp.concatenate([q_cols, k_cols, v_cols], axis=2).reshape(D, QKV_COLS)
    wo_heads = jnp.transpose(o_proj)
    normed = rms_scale(hidden.astype(jnp.float32), norm_gain).astype(jnp.bfloat16)
    query = jnp.dot(normed, jnp.transpose(q_proj), preferred_element_type=jnp.float32).reshape(BATCH, HEADS, HEAD_DIM)
    keys_new = jnp.dot(normed, jnp.transpose(k_proj), preferred_element_type=jnp.float32).reshape(BATCH, KV_HEADS, HEAD_DIM)
    values_new = jnp.dot(normed, jnp.transpose(v_proj), preferred_element_type=jnp.float32).reshape(BATCH, KV_HEADS, HEAD_DIM)
    query_rot = rotate(query, positions).astype(jnp.bfloat16)
    rotated_keys = rotate(keys_new, positions).astype(jnp.bfloat16)
    values_rot = values_new.astype(jnp.bfloat16)
    group = HEADS // KV_HEADS
    grouped_heads = query_rot.astype(jnp.float32).reshape(BATCH, KV_HEADS, group, HEAD_DIM)
    scores = jnp.einsum('bkgd,bkld->bkgl', grouped_heads, key_cache.astype(jnp.float32)) * score_scale
    capped = soft_cap * jnp.tanh(scores / soft_cap)
    valid = jnp.arange(CTX, dtype=jnp.int32)[None, :] < positions[:, None]
    weight_raw = jnp.where(valid[:, None, None, :], jnp.exp(capped), 0.0)
    self_score = lax.optimization_barrier(jnp.sum(grouped_heads * rotated_keys.astype(jnp.float32)[:, :, None, :], axis=-1)) * score_scale
    self_raw = jnp.exp(soft_cap * jnp.tanh(self_score / soft_cap))
    denom = lax.optimization_barrier(jnp.sum(weight_raw, axis=-1)) + self_raw
    weights = (weight_raw / denom[..., None]).astype(jnp.bfloat16)
    self_weight = (self_raw / denom).astype(jnp.bfloat16)
    attention = jnp.einsum('bkgl,bkld->bkgd', weights.astype(jnp.float32), value_cache.astype(jnp.float32))
    attention = attention + self_weight.astype(jnp.float32)[..., None] * values_rot.astype(jnp.float32)[:, :, None, :]
    attention = attention.reshape(BATCH, HEADS * HEAD_DIM).astype(jnp.bfloat16)
    projected = jnp.dot(attention, wo_heads, preferred_element_type=jnp.float32)
    attn_out = rms_scale(projected, post_gain).astype(jnp.bfloat16)
    return (joined_qkv, wo_heads, attn_out)
```

```python
import functools

import jax
import jax.numpy as jnp
from jax import lax
from jax.experimental import pallas as pl
from jax.experimental.pallas import tpu as pltpu
from jax.sharding import PartitionSpec as P

score_scale = 144.0 ** (-0.5)
soft_cap = 50.0


def rms_scale(values, gain):
    mean_square = jnp.mean(values * values, axis=-1, keepdims=True)
    return values * lax.rsqrt(mean_square + 1e-06) * gain


def rotate(values, positions):
    half = values.shape[-1] // 2
    freq = 10000.0 ** (-2.0 * jnp.arange(half, dtype=jnp.float32) / values.shape[-1])
    angle = positions.astype(jnp.float32)[:, None] * freq[None, :]
    cosine = jnp.cos(angle)[:, None, :]
    sine = jnp.sin(angle)[:, None, :]
    first = values[..., :half]
    second = values[..., half:]
    return jnp.concatenate(
        [first * cosine - second * sine, second * cosine + first * sine], axis=-1
    )


def join_kernel(per_tp, q_rows, k_rows, *refs):
    slot = lax.rem(lax.axis_index("rep"), per_tp)
    parts, out_ref = refs[:-1], refs[-1]
    tp_count = parts[0].shape[0]
    q_all = tp_count * per_tp * q_rows
    k_all = tp_count * per_tp * k_rows
    for step in range(per_tp):
        who = lax.rem(slot + step, per_tp)
        q_ref, kv_ref = parts[2 * step], parts[2 * step + 1]
        for start, ref, low, rows in (
            (0, q_ref, 0, q_rows),
            (q_all, kv_ref, 0, k_rows),
            (q_all + k_all, kv_ref, k_rows, k_rows),
        ):
            block = ref[:, low : low + rows, :].reshape(tp_count * rows, -1)
            at = pl.multiple_of(start + who * (tp_count * rows), 128)
            out_ref[:, pl.ds(at, tp_count * rows)] = jnp.transpose(block)


def join(per_tp, pairs):
    tp_count, q_rows, width = pairs[0][0].shape
    k_rows = pairs[0][1].shape[1] // 2
    columns = tp_count * per_tp * (q_rows + 2 * k_rows)
    stripe = 256
    operands, specs = [], []
    for pair in pairs:
        for matrix in pair:
            operands.append(matrix)
            specs.append(
                pl.BlockSpec((tp_count, matrix.shape[1], stripe), lambda j: (0, 0, j))
            )
    size = width * columns * 2
    return pl.pallas_call(
        functools.partial(join_kernel, per_tp, q_rows, k_rows),
        grid=(width // stripe,),
        in_specs=specs,
        out_specs=pl.BlockSpec((stripe, columns), lambda j: (j, 0)),
        out_shape=jax.ShapeDtypeStruct((width, columns), jnp.bfloat16),
        cost_estimate=pl.CostEstimate(flops=0, bytes_accessed=2 * size, transcendentals=0),
        name="join",
    )(*operands)


def body(
    hidden, positions, key_cache, value_cache, norm_gain, q_proj, k_proj, v_proj, o_proj, post_gain
):
    tp_count = lax.axis_size("tp")
    replica_count = lax.axis_size("rep")
    per_tp = replica_count // tp_count
    model_width = hidden.shape[1]
    q_rows, k_rows = q_proj.shape[0], k_proj.shape[0]

    groups = [[i + per_tp * p for p in range(tp_count)] for i in range(per_tp)]
    shifts = [
        [
            (per_tp * p + (i + d) % per_tp, per_tp * p + i)
            for p in range(tp_count)
            for i in range(per_tp)
        ]
        for d in range(1, per_tp)
    ]

    def collect(rows):
        planes = lax.all_gather(rows[None], "rep", axis=0, tiled=True, axis_index_groups=groups)
        return lax.all_to_all(planes, "tp", split_axis=0, concat_axis=0, tiled=True)

    kv_rows = collect(jnp.concatenate([k_proj, v_proj], axis=0))
    split_cols = o_proj.reshape(o_proj.shape[0], tp_count, -1)
    rows_of_group = lax.all_to_all(split_cols, "tp", split_axis=1, concat_axis=0, tiled=True)

    batch, kv_local, length, head_dim = key_cache.shape

    def scatter_rows(values):
        wide = values.reshape(replica_count, batch, -1)
        by_rep = lax.all_to_all(wide, "rep", split_axis=0, concat_axis=0, tiled=True)
        return by_rep

    def to_block(by_rep):
        arrived = lax.all_to_all(by_rep, "tp", split_axis=0, concat_axis=0, tiled=True)
        arrived = arrived.reshape(tp_count, per_tp, batch, -1)
        return jnp.transpose(arrived, (2, 1, 0, 3))

    normed = rms_scale(hidden.astype(jnp.float32), norm_gain).astype(jnp.bfloat16)
    normed_all = lax.all_gather(normed, "rep", axis=0, tiled=True)
    contract = (((1,), (1,)), ((), ()))
    local = jnp.concatenate(
        [
            lax.dot_general(normed_all, matrix, contract, preferred_element_type=jnp.float32)
            for matrix in (q_proj, k_proj, v_proj)
        ],
        axis=1,
    )
    block = to_block(scatter_rows(local))
    q_local = tp_count * per_tp * q_rows // head_dim
    group = q_local // kv_local
    query = block[..., :q_rows].reshape(batch, q_local, head_dim)
    keys_new = block[..., q_rows : q_rows + k_rows].reshape(batch, kv_local, head_dim)
    values_new = block[..., q_rows + k_rows :].reshape(batch, kv_local, head_dim)
    query_rot = rotate(query, positions).astype(jnp.bfloat16)
    rotated_keys = rotate(keys_new, positions).astype(jnp.bfloat16)
    values_rot = values_new.astype(jnp.bfloat16)
    grouped_heads = query_rot.reshape(batch, kv_local, group, head_dim)
    scores = (
        jnp.einsum("bkgd,bkld->bkgl", grouped_heads, key_cache, preferred_element_type=jnp.float32)
        * score_scale
    )
    capped = soft_cap * jnp.tanh(scores / soft_cap)
    valid = jnp.arange(length, dtype=jnp.int32)[None, :] < positions[:, None]
    weight_raw = jnp.where(valid[:, None, None, :], jnp.exp(capped), 0.0)
    self_score = (
        jnp.einsum("juzy,juy->juz", grouped_heads, rotated_keys, preferred_element_type=jnp.float32)
        * score_scale
    )
    self_raw = jnp.exp(soft_cap * jnp.tanh(self_score / soft_cap))
    denom = jnp.sum(weight_raw, axis=-1) + self_raw
    weights = (weight_raw / denom[..., None]).astype(jnp.bfloat16)
    self_weight = (self_raw / denom).astype(jnp.bfloat16)
    attention = jnp.einsum(
        "bkgl,bkld->bkgd", weights, value_cache, preferred_element_type=jnp.float32
    )
    attention = (
        attention
        + self_weight.astype(jnp.float32)[..., None] * values_rot.astype(jnp.float32)[:, :, None, :]
    )
    attention = attention.reshape(batch, q_local * head_dim).astype(jnp.bfloat16)
    q_later, attention = lax.optimization_barrier((q_proj, attention))
    q_own = collect(q_later)
    pairs = [(q_own, kv_rows)]
    for shift in shifts:
        pairs.append((lax.ppermute(q_own, "rep", shift), lax.ppermute(kv_rows, "rep", shift)))
    joined_block = join(per_tp, pairs)
    own_all = lax.all_gather(attention, "tp", axis=1, tiled=True)
    attention_all = lax.all_gather(own_all, "rep", axis=0, tiled=True)
    projected = lax.dot_general(
        attention_all, o_proj, contract, preferred_element_type=jnp.float32
    )
    by_rep = scatter_rows(projected)
    share = to_block(by_rep).reshape(batch, -1)
    square = jnp.sum(share * share, axis=1)
    square_all = lax.all_gather(square[None], "tp", axis=0, tiled=True)
    multiplier = lax.rsqrt(jnp.sum(square_all, axis=0) / model_width + 1e-06)
    result = share * multiplier[:, None] * post_gain
    rows_of_group, result = lax.optimization_barrier((rows_of_group, result))
    complete_rows = lax.all_gather(rows_of_group, "rep", axis=0, tiled=True)
    out_block = jnp.transpose(complete_rows.reshape(model_width, -1))
    return (joined_block, out_block, result.astype(jnp.bfloat16))


def solution(mesh):
    in_specs = (
        P("rep", None),
        P("rep"),
        P("rep", "tp", None, None),
        P("rep", "tp", None, None),
        P(),
        P(("rep", "tp"), None),
        P(("rep", "tp"), None),
        P(("rep", "tp"), None),
        P(("rep", "tp"), None),
        P("tp"),
    )
    out_specs = (P(None, "tp"), P("tp", None), P("rep", "tp"))
    return jax.shard_map(body, mesh=mesh, in_specs=in_specs, out_specs=out_specs, check_vma=False)
```

```python
import functools

import jax
import jax.numpy as jnp
from jax import lax
from jax.experimental import pallas as pl
from jax.experimental.pallas import tpu as pltpu
from jax.sharding import PartitionSpec as P

score_scale = 144.0 ** (-0.5)
soft_cap = 50.0


def rms_scale(values, gain):
    mean_square = jnp.mean(values * values, axis=-1, keepdims=True)
    return values * lax.rsqrt(mean_square + 1e-06) * gain


def rotate(values, positions):
    half = values.shape[-1] // 2
    freq = 10000.0 ** (-2.0 * jnp.arange(half, dtype=jnp.float32) / values.shape[-1])
    angle = positions.astype(jnp.float32)[:, None] * freq[None, :]
    cosine = jnp.cos(angle)[:, None, :]
    sine = jnp.sin(angle)[:, None, :]
    first = values[..., :half]
    second = values[..., half:]
    return jnp.concatenate(
        [first * cosine - second * sine, second * cosine + first * sine], axis=-1
    )


def join_kernel(per_tp, q_rows, k_rows, *refs):
    slot = lax.rem(lax.axis_index("rep"), per_tp)
    parts, out_ref = refs[:-1], refs[-1]
    tp_count = parts[0].shape[0]
    q_all = tp_count * per_tp * q_rows
    k_all = tp_count * per_tp * k_rows
    for step in range(per_tp):
        who = lax.rem(slot + step, per_tp)
        q_ref, kv_ref = parts[2 * step], parts[2 * step + 1]
        for start, ref, low, rows in (
            (0, q_ref, 0, q_rows),
            (q_all, kv_ref, 0, k_rows),
            (q_all + k_all, kv_ref, k_rows, k_rows),
        ):
            block = ref[:, low : low + rows, :].reshape(tp_count * rows, -1)
            at = pl.multiple_of(start + who * (tp_count * rows), 128)
            out_ref[:, pl.ds(at, tp_count * rows)] = jnp.transpose(block)


def join(per_tp, pairs):
    tp_count, q_rows, width = pairs[0][0].shape
    k_rows = pairs[0][1].shape[1] // 2
    columns = tp_count * per_tp * (q_rows + 2 * k_rows)
    stripe = 256
    operands, specs = [], []
    for pair in pairs:
        for matrix in pair:
            operands.append(matrix)
            specs.append(
                pl.BlockSpec((tp_count, matrix.shape[1], stripe), lambda j: (0, 0, j))
            )
    size = width * columns * 2
    return pl.pallas_call(
        functools.partial(join_kernel, per_tp, q_rows, k_rows),
        grid=(width // stripe,),
        in_specs=specs,
        out_specs=pl.BlockSpec((stripe, columns), lambda j: (j, 0)),
        out_shape=jax.ShapeDtypeStruct((width, columns), jnp.bfloat16),
        cost_estimate=pl.CostEstimate(flops=0, bytes_accessed=2 * size, transcendentals=0),
        name="join",
    )(*operands)


def turn_kernel(rows_ref, out_ref):
    out_ref[...] = jnp.transpose(rows_ref[...])


def turn(rows):
    height, width = rows.shape
    stripe = 384 if height % 384 == 0 else 128
    return pl.pallas_call(
        turn_kernel,
        grid=(height // stripe,),
        in_specs=[pl.BlockSpec((stripe, width), lambda j: (j, 0))],
        out_specs=pl.BlockSpec((width, stripe), lambda j: (0, j)),
        out_shape=jax.ShapeDtypeStruct((width, height), rows.dtype),
        cost_estimate=pl.CostEstimate(
            flops=0, bytes_accessed=4 * height * width, transcendentals=0
        ),
        name="turn",
    )(rows)


def body(
    hidden, positions, key_cache, value_cache, norm_gain, q_proj, k_proj, v_proj, o_proj, post_gain
):
    tp_count = lax.axis_size("tp")
    replica_count = lax.axis_size("rep")
    per_tp = replica_count // tp_count
    model_width = hidden.shape[1]
    q_rows, k_rows = q_proj.shape[0], k_proj.shape[0]

    groups = [[i + per_tp * p for p in range(tp_count)] for i in range(per_tp)]
    shifts = [
        [
            (per_tp * p + (i + d) % per_tp, per_tp * p + i)
            for p in range(tp_count)
            for i in range(per_tp)
        ]
        for d in range(1, per_tp)
    ]

    def collect(rows):
        planes = lax.all_gather(rows[None], "rep", axis=0, tiled=True, axis_index_groups=groups)
        return lax.all_to_all(planes, "tp", split_axis=0, concat_axis=0, tiled=True)

    kv_rows = collect(jnp.concatenate([k_proj, v_proj], axis=0))
    split_cols = o_proj.reshape(o_proj.shape[0], tp_count, -1)
    rows_of_group = lax.all_to_all(split_cols, "tp", split_axis=1, concat_axis=0, tiled=True)

    batch, kv_local, length, head_dim = key_cache.shape

    def scatter_rows(values):
        wide = values.reshape(replica_count, batch, -1)
        by_rep = lax.all_to_all(wide, "rep", split_axis=0, concat_axis=0, tiled=True)
        return by_rep

    def to_block(by_rep):
        arrived = lax.all_to_all(by_rep, "tp", split_axis=0, concat_axis=0, tiled=True)
        arrived = arrived.reshape(tp_count, per_tp, batch, -1)
        return jnp.transpose(arrived, (2, 1, 0, 3))

    normed = rms_scale(hidden.astype(jnp.float32), norm_gain).astype(jnp.bfloat16)
    normed_all = lax.all_gather(normed, "rep", axis=0, tiled=True)
    contract = (((1,), (1,)), ((), ()))
    local = jnp.concatenate(
        [
            lax.dot_general(normed_all, matrix, contract, preferred_element_type=jnp.float32)
            for matrix in (q_proj, k_proj, v_proj)
        ],
        axis=1,
    )
    block = to_block(scatter_rows(local))
    q_local = tp_count * per_tp * q_rows // head_dim
    group = q_local // kv_local
    query = block[..., :q_rows].reshape(batch, q_local, head_dim)
    keys_new = block[..., q_rows : q_rows + k_rows].reshape(batch, kv_local, head_dim)
    values_new = block[..., q_rows + k_rows :].reshape(batch, kv_local, head_dim)
    query_rot = rotate(query, positions).astype(jnp.bfloat16)
    rotated_keys = rotate(keys_new, positions).astype(jnp.bfloat16)
    values_rot = values_new.astype(jnp.bfloat16)
    grouped_heads = query_rot.reshape(batch, kv_local, group, head_dim)
    scores = (
        jnp.einsum("bkgd,bkld->bkgl", grouped_heads, key_cache, preferred_element_type=jnp.float32)
        * score_scale
    )
    capped = soft_cap * jnp.tanh(scores / soft_cap)
    valid = jnp.arange(length, dtype=jnp.int32)[None, :] < positions[:, None]
    weight_raw = jnp.where(valid[:, None, None, :], jnp.exp(capped), 0.0)
    self_score = (
        jnp.einsum("juzy,juy->juz", grouped_heads, rotated_keys, preferred_element_type=jnp.float32)
        * score_scale
    )
    self_raw = jnp.exp(soft_cap * jnp.tanh(self_score / soft_cap))
    denom = jnp.sum(weight_raw, axis=-1) + self_raw
    weights = (weight_raw / denom[..., None]).astype(jnp.bfloat16)
    self_weight = (self_raw / denom).astype(jnp.bfloat16)
    attention = jnp.einsum(
        "bkgl,bkld->bkgd", weights, value_cache, preferred_element_type=jnp.float32
    )
    attention = (
        attention
        + self_weight.astype(jnp.float32)[..., None] * values_rot.astype(jnp.float32)[:, :, None, :]
    )
    attention = attention.reshape(batch, q_local * head_dim).astype(jnp.bfloat16)
    q_later, attention = lax.optimization_barrier((q_proj, attention))
    q_own = collect(q_later)
    pairs = [(q_own, kv_rows)]
    for shift in shifts:
        pairs.append((lax.ppermute(q_own, "rep", shift), lax.ppermute(kv_rows, "rep", shift)))
    joined_block = join(per_tp, pairs)
    own_all = lax.all_gather(attention, "tp", axis=1, tiled=True)
    attention_all = lax.all_gather(own_all, "rep", axis=0, tiled=True)
    projected = lax.dot_general(
        attention_all, o_proj, contract, preferred_element_type=jnp.float32
    )
    by_rep = scatter_rows(projected)
    share = to_block(by_rep).reshape(batch, -1)
    square = jnp.sum(share * share, axis=1)
    square_all = lax.all_gather(square[None], "tp", axis=0, tiled=True)
    multiplier = lax.rsqrt(jnp.sum(square_all, axis=0) / model_width + 1e-06)
    result = share * multiplier[:, None] * post_gain
    rows_of_group, result = lax.optimization_barrier((rows_of_group, result))
    complete_rows = lax.all_gather(rows_of_group, "rep", axis=0, tiled=True)
    out_block = turn(complete_rows.reshape(model_width, -1))
    return (joined_block, out_block, result.astype(jnp.bfloat16))


def solution(mesh):
    in_specs = (
        P("rep", None),
        P("rep"),
        P("rep", "tp", None, None),
        P("rep", "tp", None, None),
        P(),
        P(("rep", "tp"), None),
        P(("rep", "tp"), None),
        P(("rep", "tp"), None),
        P(("rep", "tp"), None),
        P("tp"),
    )
    out_specs = (P(None, "tp"), P("tp", None), P("rep", "tp"))
    return jax.shard_map(body, mesh=mesh, in_specs=in_specs, out_specs=out_specs, check_vma=False)
```
